16 devices in a mesh: batch: 2 (over z), row: 8 (over y, x, core).
Axes of the slice: x: 2, y: 2, z: 2, core: 2. Of those that a mesh axis runs over, the one named last changes fastest.
Arguments:
- trans_mat: bfloat16 [32768, 16384], P(('batch', 'row')), parts along dimension 0
- teleport: float32 [32768, 256], P(('batch', 'row')), parts along dimension 0
- dangling: int32 [32768], P(('batch', 'row')), parts along dimension 0
- damping: float32 [8], replicated
- rank_init: float32 [32768, 256], P(('batch', 'row')), parts along dimension 0
Outputs:
- output: float32 [32768, 256], P(('batch', 'row')), parts along dimension 0
There are 2 independent parts. The reference program is written for one: setup_inputs(seed, part) draws one part's arguments, and reference() takes and returns one part's arrays. A program takes and returns all parts, laid end to end along the dimension named above; an argument that names none is the same for every part.
All inputs are finite; a program needn't handle non-finite values.
Results may differ from the reference program's by a relative error of at most 0.001.
Values are sent between devices in bfloat16 or wider.
A program may use at most 1 GiB of HBM per device.

```python
import jax
import jax.numpy as jnp
from jax import lax

NODES = 16384
SEEDS = 256
SWEEPS = 8


def setup_inputs(seed: int = 0, part: int = 0) -> dict:
    base_key = jax.random.key(seed)
    part_key = jax.random.fold_in(base_key, part)
    key_list = jax.random.split(part_key, 8)
    dangling = (jax.random.randint(key_list[0], (NODES,), 0, 100) < 20).astype(jnp.int32)
    popular = jnp.exp(0.8 * jax.random.normal(key_list[1], (NODES,), jnp.float32))
    weights = popular[:, None] * jnp.maximum(jax.random.uniform(key_list[2], (NODES, NODES), jnp.float32) - 0.5, 0.0)
    keep_cols = 1.0 - dangling.astype(jnp.float32)
    col_sum = jnp.sum(weights, axis=0)
    trans_mat = (weights * (keep_cols / jnp.maximum(col_sum, 1e-6))[None, :]).astype(jnp.bfloat16)
    tele_raw = jnp.exp(1.2 * jax.random.normal(key_list[3], (NODES, SEEDS), jnp.float32))
    teleport = tele_raw / jnp.mean(tele_raw, axis=0, keepdims=True)
    col_scale = jax.random.uniform(key_list[4], (1, SEEDS), jnp.float32, 0.3, 3.0)
    rank_init = col_scale * jax.random.uniform(key_list[5], (NODES, SEEDS), jnp.float32, 0.2, 1.8)
    damping = jax.random.uniform(jax.random.key(seed + 1), (SWEEPS,), jnp.float32, 0.75, 0.95)
    return {"trans_mat": trans_mat, "teleport": teleport, "dangling": dangling, "damping": damping, "rank_init": rank_init}


def reference(trans_mat, teleport, dangling, damping, rank_init):
    dang_float = dangling.astype(jnp.float32)

    def one_sweep(rank_cur, factor):
        prod_rows = jnp.dot(trans_mat, rank_cur.astype(jnp.bfloat16), preferred_element_type=jnp.float32)
        dang_mass = jnp.dot(dang_float, rank_cur, preferred_element_type=jnp.float32)
        rank_next = factor * prod_rows + (1.0 - factor) * teleport + (factor / NODES) * dang_mass[None, :]
        return rank_next, None

    rank_final, unused = lax.scan(one_sweep, rank_init, damping)
    return rank_final
```

```python
import functools

import jax
import jax.numpy as jnp
from jax import lax
from jax.experimental import pallas as pl
from jax.experimental.pallas import tpu as pltpu
from jax.sharding import PartitionSpec as P

MESH = pl.DeviceIdType.MESH
OWN, SIB, XN, XS, YN, YS, DG, DS = range(8)
X_OWN, Y_OWN, X_FWD, Y_FWD, S_OWN, S_X, S_Y, S_D = range(8)
RING = 12
UNITS = 24
KU = 512
KF = 256


def flip(a, b):
    return a + b - 2 * a * b


def kernel(num_sweeps, a_hbm, e_hbm, d_hbm, damp, r_hbm, out_hbm, g, ring, res, acc, ev, dcol, dbuf, mass,
           recv, send, mrecv, msend, ring_sem, res_sem, io_sem):
    rows = acc.shape[1]
    nodes = a_hbm.shape[1]
    group = lax.axis_index("batch")
    me = lax.axis_index("row")
    core = lax.rem(me, 2)
    xpos = lax.rem(lax.div(me, 2), 2)
    ypos = lax.div(me, 4)

    def index_of(sbit, xbit, ybit):
        return (flip(ypos, ybit) * 2 + flip(xpos, xbit)) * 2 + flip(core, sbit)

    def peer(slot):
        return (group, index_of(slot & 1, (slot >> 1) & 1, (slot >> 2) & 1))

    def remote(kind, p, h, c, src, dst):
        to = {X_OWN: XN, Y_OWN: YN, X_FWD: XN, Y_FWD: YN}.get(kind, SIB)
        return pltpu.make_async_remote_copy(src_ref=src, dst_ref=dst, send_sem=send.at[kind, p, h],
                                            recv_sem=recv.at[kind, p, h, c], device_id=peer(to), device_id_type=MESH)

    def block_copy(kind, p, h, c):
        src, dst = {X_OWN: (OWN, XN), Y_OWN: (OWN, YN), S_OWN: (OWN, SIB), S_X: (XN, XS), S_Y: (YN, YS),
                    S_D: (DG, DS)}[kind]
        at = pl.ds(pl.multiple_of(c * KU, KU), KU)
        return remote(kind, p, h, c, g.at[p, h, src, at], g.at[p, h, dst, at])

    def relay_copy(kind, p, h, f):
        src, start, part = (YN, 0, 0) if kind == X_FWD else (XN, rows // 2, KF)
        return remote(kind, p, h, f, g.at[p, h, src, pl.ds(start + f * KF, KF)],
                      g.at[p, h, DG, pl.ds(f * KU + part, KF)])

    def wait_relay(kind, p, h, f):
        part = 0 if kind == X_FWD else KF
        at = g.at[p, h, DG, pl.ds(pl.multiple_of(f * KU + part, KF), KF)]
        remote(kind, p, h, f, at, at).wait_recv()

    def wait_sends(p, h):
        for kind in range(8):
            size = rows // 2 if kind in (X_FWD, Y_FWD) else rows
            at = g.at[p, h, OWN, pl.ds(0, size)]
            remote(kind, p, h, 0, at, at).wait_send()

    def unit_copy(u):
        late = lax.div(lax.div(u, 8) + 1, 2)
        w = u - 8 * late
        early = 1 - late
        i = lax.rem(w, 4)
        j = lax.div(w, 4)
        sbit = early * j + late * lax.div(i, 2)
        ybit = late * lax.rem(i, 2)
        xbit = late * (1 - lax.rem(i, 2))
        part = early * i + late * j
        col = pl.multiple_of(index_of(sbit, xbit, ybit) * rows + part * KU, KU)
        slot = lax.rem(u, RING)
        return pltpu.make_async_copy(a_hbm.at[:, pl.ds(col, KU)], ring.at[slot], ring_sem.at[slot])

    def res_copy(i, f, part):
        col = pl.multiple_of(index_of(i, 1, 1) * rows + f * KF + part * (rows // 2), KF)
        return pltpu.make_async_copy(a_hbm.at[:, pl.ds(col, KF)], res.at[i, f, :, pl.ds(part * KF, KF)],
                                     res_sem.at[i, f, part])

    def half_copy(src, dst, h, sem):
        return pltpu.make_async_copy(src.at[:, pl.ds(h * 128, 128)], dst.at[h], sem)

    for h in range(2):
        half_copy(r_hbm, acc, h, io_sem.at[h]).start()
    d_copy = pltpu.make_async_copy(d_hbm, dbuf, io_sem.at[4])
    d_copy.start()

    @pl.loop(0, RING)
    def _(u):
        unit_copy(u).start()

    for h in range(2):
        half_copy(e_hbm, ev, h, io_sem.at[2 + h]).start()
    for i in range(2):
        for f in range(4):
            for part in range(2):
                res_copy(i, f, part).start()

    barrier = pltpu.get_barrier_semaphore()
    for slot in range(1, 8):
        pl.semaphore_signal(barrier, inc=1, device_id=peer(slot), device_id_type=MESH)
    pl.semaphore_wait(barrier, 7)

    def send_own(p, h, c):
        for kind in (X_OWN, Y_OWN, S_OWN):
            block_copy(kind, p, h, c).start()

    def mass_copy(p, h, slot):
        return pltpu.make_async_remote_copy(src_ref=mass.at[p, h, 0], dst_ref=mass.at[p, h, slot],
                                            send_sem=msend.at[p, h], recv_sem=mrecv.at[p, h, slot],
                                            device_id=peer(slot), device_id_type=MESH)

    def send_mass(p, h, part):
        mass[p, h, 0] = jnp.sum(part, axis=0, keepdims=True)
        for slot in range(1, 8):
            mass_copy(p, h, slot).start()

    def wait_mass_sends(p, h):
        at = mass.at[p, h, pl.ds(0, 7)]
        pltpu.make_async_remote_copy(src_ref=at, dst_ref=at, send_sem=msend.at[p, h], recv_sem=mrecv.at[p, h, 0],
                                     device_id=peer(SIB), device_id_type=MESH).wait_send()

    def fold(c, value):
        weighed = value * dcol[pl.ds(c * KU, KU), :]
        return jnp.sum(weighed.reshape(KU // 8, 8, 128), axis=0)

    for h in range(2):
        half_copy(r_hbm, acc, h, io_sem.at[h]).wait()
        for c in range(4):
            at = pl.ds(c * KU, KU)
            g[0, h, OWN, at] = acc[h, at].astype(jnp.bfloat16)
            if c:
                send_own(0, h, c - 1)
        send_own(0, h, 3)

    d_copy.wait()
    for c in range(rows // 128):
        line = jnp.broadcast_to(dbuf[pl.ds(c, 1), :].astype(jnp.float32), (128, 128))
        dcol[pl.ds(c * 128, 128), :] = line.T
    for h in range(2):
        part = jnp.zeros((8, 128), jnp.float32)
        for c in range(4):
            part += fold(c, acc[h, pl.ds(c * KU, KU)])
        send_mass(0, h, part)
        acc[h] = jnp.zeros_like(acc[h])

    for h in range(2):
        half_copy(e_hbm, ev, h, io_sem.at[2 + h]).wait()
    for i in range(2):
        for f in range(4):
            for part in range(2):
                res_copy(i, f, part).wait()

    def sweep(t, carry):
        p = lax.rem(t, 2)
        q = 1 - p
        more = t < num_sweeps - 1
        factor = damp[t]

        def wide(u, slot, c):
            unit_copy(u).wait()
            at = pl.ds(pl.multiple_of(c * KU, KU), KU)
            piece = jnp.concatenate([g[p, 0, slot, at], g[p, 1, slot, at]], axis=1)
            buf = ring.at[lax.rem(u, RING)]
            for m in range(rows // KU):
                mt = pl.ds(m * KU, KU)
                prod = jnp.dot(buf[mt], piece, preferred_element_type=jnp.float32)
                acc[0, mt] += prod[:, :128]
                acc[1, mt] += prod[:, 128:]

            @pl.when((u < RING) | more)
            def _():
                unit_copy(lax.rem(u + RING, UNITS)).start()

        @pl.loop(0, 4)
        def _(c):
            wide(c, OWN, c)

        @pl.loop(0, 4)
        def _(c):
            for h in range(2):
                block_copy(S_OWN, p, h, c).wait_recv()
            wide(c + 4, SIB, c)

        @pl.loop(0, 4)
        def _(c):
            for h in range(2):
                block_copy(X_OWN, p, h, c).wait_recv()
                block_copy(S_X, p, h, c).start()
                block_copy(Y_OWN, p, h, c).wait_recv()
                block_copy(S_Y, p, h, c).start()
                for kind, base in ((X_FWD, 0), (Y_FWD, 2)):
                    if h == 0:
                        for half in range(2):
                            @pl.when(c == base + half)
                            def _():
                                relay_copy(kind, p, 0, 2 * half).start()
                                relay_copy(kind, p, 0, 2 * half + 1).start()
                    else:
                        @pl.when(c == base + 1)
                        def _():
                            for f in range(4):
                                relay_copy(kind, p, 1, f).start()
            wide(4 * c + 8, XN, c)
            wide(4 * c + 9, YN, c)
            for h in range(2):
                block_copy(S_X, p, h, c).wait_recv()
            wide(4 * c + 10, XS, c)
            for h in range(2):
                block_copy(S_Y, p, h, c).wait_recv()
            wide(4 * c + 11, YS, c)

        @pl.loop(0, 2)
        def _(h):
            def narrow(i, f):
                at = pl.ds(pl.multiple_of(f * KU, KU), KU)
                piece = g[p, h, DG + i, at]
                for m in range(rows // KU):
                    mt = pl.ds(m * KU, KU)
                    acc[h, mt] += jnp.dot(res[i, f, mt], piece, preferred_element_type=jnp.float32)

            @pl.loop(0, 4)
            def _(f):
                wait_relay(X_FWD, p, h, f)
                wait_relay(Y_FWD, p, h, f)
                block_copy(S_D, p, h, f).start()

                @pl.when(f > 0)
                def _():
                    block_copy(S_D, p, h, f - 1).wait_recv()
                    narrow(1, f - 1)

                narrow(0, f)

            block_copy(S_D, p, h, 3).wait_recv()
            narrow(1, 3)

            for slot in range(1, 8):
                mass_copy(p, h, slot).wait_recv()
            line = (factor / nodes) * jnp.sum(mass[p, h], axis=0)

            def next_rows(c):
                at = pl.ds(c * KU, KU)
                return factor * acc[h, at] + (1.0 - factor) * ev[h, at] + line

            @pl.when(more)
            def _():
                part = jnp.zeros((8, 128), jnp.float32)
                for c in range(4):
                    at = pl.ds(c * KU, KU)
                    value = next_rows(c)
                    g[q, h, OWN, at] = value.astype(jnp.bfloat16)
                    part += fold(c, value)
                    acc[h, at] = jnp.zeros((KU, 128), jnp.float32)
                    if c:
                        send_own(q, h, c - 1)
                wait_sends(p, h)
                wait_mass_sends(p, h)
                send_own(q, h, 3)
                send_mass(q, h, part)

            @pl.when(jnp.logical_not(more))
            def _():
                for c in range(4):
                    acc[h, pl.ds(c * KU, KU)] = next_rows(c)
                pltpu.make_async_copy(acc.at[h], out_hbm.at[:, pl.ds(pl.multiple_of(h * 128, 128), 128)],
                                      io_sem.at[5 + h]).start()
                wait_sends(p, h)
                wait_mass_sends(p, h)

        return carry

    lax.fori_loop(0, num_sweeps, sweep, 0)
    for h in range(2):
        pltpu.make_async_copy(acc.at[h], out_hbm.at[:, pl.ds(h * 128, 128)], io_sem.at[5 + h]).wait()


def solution(mesh):
    spec_rows = P(("batch", "row"), None)
    spec_vec = P(("batch", "row"))

    def local_sweeps(mat_rows, tele_rows, dang_rows, damping, start_rows):
        rows, nodes = mat_rows.shape
        seeds = start_rows.shape[1]
        num_sweeps = damping.shape[0]
        any_space = pl.BlockSpec(memory_space=pl.ANY)
        sem = pltpu.SemaphoreType.DMA
        return pl.pallas_call(
            functools.partial(kernel, num_sweeps),
            out_shape=jax.ShapeDtypeStruct((rows, seeds), jnp.float32),
            in_specs=[any_space, any_space, any_space, pl.BlockSpec(memory_space=pltpu.SMEM), any_space],
            out_specs=any_space,
            scratch_shapes=[
                pltpu.VMEM((2, 2, 8, rows, 128), jnp.bfloat16),
                pltpu.VMEM((RING, rows, KU), jnp.bfloat16),
                pltpu.VMEM((2, 4, rows, KU), jnp.bfloat16),
                pltpu.VMEM((2, rows, 128), jnp.float32),
                pltpu.VMEM((2, rows, 128), jnp.float32),
                pltpu.VMEM((rows, 128), jnp.float32),
                pltpu.VMEM((rows // 128, 128), jnp.int32),
                pltpu.VMEM((2, 2, 8, 1, 128), jnp.float32),
                sem((8, 2, 2, 4)),
                sem((8, 2, 2)),
                sem((2, 2, 8)),
                sem((2, 2)),
                sem((RING,)),
                sem((2, 4, 2)),
                sem((7,)),
            ],
            compiler_params=pltpu.CompilerParams(collective_id=0, has_side_effects=True, vmem_limit_bytes=67043328),
            name="sweeps",
        )(mat_rows, tele_rows, dang_rows.reshape(rows // 128, 128), damping, start_rows)

    return jax.shard_map(local_sweeps, mesh=mesh, in_specs=(spec_rows, spec_rows, spec_vec, P(None), spec_rows),
                         out_specs=spec_rows, check_vma=False)
```

```python
import functools

import jax
import jax.numpy as jnp
from jax import lax
from jax.experimental import pallas as pl
from jax.experimental.pallas import tpu as pltpu
from jax.sharding import PartitionSpec as P

MESH = pl.DeviceIdType.MESH
OWN, SIB, XN, XS, YN, YS, DG, DS = range(8)
X_OWN, Y_OWN, X_FWD, Y_FWD, S_OWN, S_X, S_Y, S_D = range(8)
RING = 6
UNITS = 12
KU = 512
KF = 256
MB = 512
NEAR = (SIB, XN, YN)
KERNEL_VMEM = 64487424


def flip(a, b):
    return a + b - 2 * a * b


def kernel(num_sweeps, a_hbm, e_hbm, d_hbm, damp, r_hbm, acc, g, ring, res, ev, dcol, dbuf, mass,
           recv, send, mrecv, msend, ring_sem, res_sem, io_sem, ready):
    rows = acc.shape[1]
    nodes = a_hbm.shape[1]
    group = lax.axis_index("batch")
    me = lax.axis_index("row")
    core = lax.rem(me, 2)
    xpos = lax.rem(lax.div(me, 2), 2)
    ypos = lax.div(me, 4)

    def index_of(slot):
        sbit, xbit, ybit = slot & 1, (slot >> 1) & 1, (slot >> 2) & 1
        return (flip(ypos, ybit) * 2 + flip(xpos, xbit)) * 2 + flip(core, sbit)

    def peer(slot):
        return (group, index_of(slot))

    barrier = pltpu.get_barrier_semaphore()
    for slot in NEAR:
        pl.semaphore_signal(barrier, inc=1, device_id=peer(slot), device_id_type=MESH)

    def remote(kind, p, h, c, src, dst):
        to = {X_OWN: XN, Y_OWN: YN, X_FWD: XN, Y_FWD: YN}.get(kind, SIB)
        return pltpu.make_async_remote_copy(src_ref=src, dst_ref=dst, send_sem=send.at[kind, p, h],
                                            recv_sem=recv.at[kind, p, h, c], device_id=peer(to), device_id_type=MESH)

    def block_copy(kind, p, h, c):
        src, dst = {X_OWN: (OWN, XN), Y_OWN: (OWN, YN), S_OWN: (OWN, SIB), S_X: (XN, XS), S_Y: (YN, YS),
                    S_D: (DG, DS)}[kind]
        at = pl.ds(pl.multiple_of(c * KU, KU), KU)
        return remote(kind, p, h, c, g.at[p, h, src, at], g.at[p, h, dst, at])

    def relay_copy(kind, p, h, f):
        src, start, part = (YN, 0, 0) if kind == X_FWD else (XN, rows // 2, KF)
        return remote(kind, p, h, f, g.at[p, h, src, pl.ds(start + f * KF, KF)],
                      g.at[p, h, DG, pl.ds(f * KU + part, KF)])

    def wait_relay(kind, p, h, f):
        part = 0 if kind == X_FWD else KF
        at = g.at[p, h, DG, pl.ds(pl.multiple_of(f * KU + part, KF), KF)]
        remote(kind, p, h, f, at, at).wait_recv()

    def wait_sends(p, h):
        for kind in range(8):
            size = rows // 2 if kind in (X_FWD, Y_FWD) else rows
            at = g.at[p, h, OWN, pl.ds(0, size)]
            remote(kind, p, h, 0, at, at).wait_send()

    def parts_of(u):
        if u < 4:
            return [(u // 2, 2 * (u % 2)), (u // 2, 2 * (u % 2) + 1)]
        return [(slot, (u - 4) // 2) for slot in ((XN, YN) if u % 2 == 0 else (XS, YS))]

    def start_unit(u):
        parts = parts_of(u)
        if parts[0][0] == parts[1][0]:
            parts = [(parts[0][0], parts[0][1], 0, 2 * KU)]
        else:
            parts = [(slot, c, i * KU, KU) for i, (slot, c) in enumerate(parts)]
        for slot, c, to, size in parts:
            col = pl.multiple_of(index_of(slot) * rows + c * KU, KU)
            pltpu.make_async_copy(a_hbm.at[:, pl.ds(col, size)], ring.at[u % RING, :, pl.ds(to, size)],
                                  ring_sem.at[u % RING]).start()

    def wait_unit(u):
        at = ring.at[u % RING]
        pltpu.make_async_copy(at, at, ring_sem.at[u % RING]).wait()

    def res_copy(i, f, part):
        col = pl.multiple_of(index_of(DG + i) * rows + f * KF + part * (rows // 2), KF)
        return pltpu.make_async_copy(a_hbm.at[:, pl.ds(col, KF)], res.at[i, f, :, pl.ds(part * KF, KF)],
                                     res_sem.at[i, f, part])

    def half_copy(src, dst, h, sem):
        return pltpu.make_async_copy(src.at[:, pl.ds(h * 128, 128)], dst.at[h], sem)

    for h in range(2):
        half_copy(r_hbm, acc, h, io_sem.at[h]).start()
    d_copy = pltpu.make_async_copy(d_hbm, dbuf, io_sem.at[4])
    d_copy.start()
    pl.semaphore_wait(barrier, 3)

    def send_own(p, h, c):
        for kind in (X_OWN, Y_OWN, S_OWN):
            block_copy(kind, p, h, c).start()

    def mass_copy(p, h, slot):
        return pltpu.make_async_remote_copy(src_ref=mass.at[p, h, 0], dst_ref=mass.at[p, h, slot],
                                            send_sem=msend.at[p, h], recv_sem=mrecv.at[p, h, slot],
                                            device_id=peer(slot), device_id_type=MESH)

    def send_mass(p, h, part):
        mass[p, h, 0] = jnp.sum(part, axis=0, keepdims=True)
        for slot in range(1, 8):
            mass_copy(p, h, slot).start()

    def wait_mass_sends(p, h):
        at = mass.at[p, h, pl.ds(0, 7)]
        pltpu.make_async_remote_copy(src_ref=at, dst_ref=at, send_sem=msend.at[p, h], recv_sem=mrecv.at[p, h, 0],
                                     device_id=peer(SIB), device_id_type=MESH).wait_send()

    def fold(c, value):
        weighed = value * dcol[pl.ds(c * KU, KU), :]
        return jnp.sum(weighed.reshape(KU // 8, 8, 128), axis=0)

    for h in range(2):
        half_copy(r_hbm, acc, h, io_sem.at[h]).wait()
        for c in range(4):
            at = pl.ds(c * KU, KU)
            g[0, h, OWN, at] = acc[h, at].astype(jnp.bfloat16)
            if h == 0 and c in (1, 2):
                send_own(0, 0, c - 1)
    for h, c in ((1, 0), (1, 1), (0, 2), (1, 2), (0, 3), (1, 3)):
        send_own(0, h, c)

    for u in range(RING):
        start_unit(u)
    for h in range(2):
        half_copy(e_hbm, ev, h, io_sem.at[2 + h]).start()
    for i in range(2):
        for f in range(4):
            for part in range(2):
                res_copy(i, f, part).start()
    for slot in NEAR:
        pl.semaphore_signal(ready.at[0], inc=1, device_id=peer(slot), device_id_type=MESH)
    d_copy.wait()
    for c in range(rows // 128):
        line = jnp.broadcast_to(dbuf[pl.ds(c, 1), :].astype(jnp.float32), (128, 128))
        dcol[pl.ds(c * 128, 128), :] = line.T
    pl.semaphore_wait(ready.at[0], 3)
    for slot in NEAR:
        pl.semaphore_signal(ready.at[1], inc=1, device_id=peer(slot), device_id_type=MESH)
    sums = []
    for h in range(2):
        part = jnp.zeros((8, 128), jnp.float32)
        for c in range(4):
            part += fold(c, acc[h, pl.ds(c * KU, KU)])
        sums.append(part)
        acc[h] = jnp.zeros_like(acc[h])
    pl.semaphore_wait(ready.at[1], 3)
    for h in range(2):
        send_mass(0, h, sums[h])

    def sweep(t, carry):
        p = lax.rem(t, 2)
        q = 1 - p
        more = t < num_sweeps - 1
        factor = damp[t]

        def wide(u):
            wait_unit(u)
            piece = jnp.concatenate(
                [jnp.concatenate([g[p, h, slot, pl.ds(c * KU, KU)] for h in range(2)], axis=1) for slot, c in parts_of(u)],
                axis=0)
            for m in range(rows // MB):
                mt = pl.ds(m * MB, MB)
                prod = jnp.dot(ring[u % RING, mt], piece, preferred_element_type=jnp.float32)
                acc[0, mt] += prod[:, :128]
                acc[1, mt] += prod[:, 128:]
            if u + RING < UNITS:
                start_unit(u + RING)
            else:
                @pl.when(more)
                def _():
                    start_unit(u + RING - UNITS)

        wide(0)
        wide(1)
        for u in (2, 3):
            for slot, c in parts_of(u):
                for h in range(2):
                    block_copy(S_OWN, p, h, c).wait_recv()
            wide(u)
        for c in range(4):
            for h in range(2):
                block_copy(X_OWN, p, h, c).wait_recv()
                block_copy(S_X, p, h, c).start()
                block_copy(Y_OWN, p, h, c).wait_recv()
                block_copy(S_Y, p, h, c).start()
                kind = X_FWD if c < 2 else Y_FWD
                for f in ((2 * (c % 2), 2 * (c % 2) + 1) if h == 0 else range(4 * (c % 2))):
                    relay_copy(kind, p, h, f).start()
            wide(2 * c + 4)
            for h in range(2):
                block_copy(S_X, p, h, c).wait_recv()
                block_copy(S_Y, p, h, c).wait_recv()
            wide(2 * c + 5)

        @pl.when(t == 0)
        def _():
            for h in range(2):
                half_copy(e_hbm, ev, h, io_sem.at[2 + h]).wait()
            for i in range(2):
                for f in range(4):
                    for part in range(2):
                        res_copy(i, f, part).wait()

        for h in range(2):
            def narrow(*terms):
                pieces = [g[p, h, DG + i, pl.ds(pl.multiple_of(f * KU, KU), KU)] for i, f in terms]
                piece = jnp.concatenate(pieces, axis=0) if len(terms) > 1 else pieces[0]
                for m in range(rows // MB):
                    mt = pl.ds(m * MB, MB)
                    left = [res[i, f, mt] for i, f in terms]
                    left = jnp.concatenate(left, axis=1) if len(terms) > 1 else left[0]
                    acc[h, mt] += jnp.dot(left, piece, preferred_element_type=jnp.float32)

            def take(f):
                wait_relay(X_FWD, p, h, f)
                wait_relay(Y_FWD, p, h, f)
                block_copy(S_D, p, h, f).start()

            take(0)
            narrow((0, 0))

            @pl.loop(1, 4)
            def _(f):
                take(f)
                block_copy(S_D, p, h, f - 1).wait_recv()
                narrow((0, f), (1, f - 1))

            block_copy(S_D, p, h, 3).wait_recv()
            narrow((1, 3))

            for slot in range(1, 8):
                mass_copy(p, h, slot).wait_recv()
            line = (factor / nodes) * jnp.sum(mass[p, h], axis=0)

            def next_rows(c):
                at = pl.ds(c * KU, KU)
                return factor * acc[h, at] + (1.0 - factor) * ev[h, at] + line

            @pl.when(more)
            def _():
                part = jnp.zeros((8, 128), jnp.float32)
                for c in range(4):
                    at = pl.ds(c * KU, KU)
                    value = next_rows(c)
                    g[q, h, OWN, at] = value.astype(jnp.bfloat16)
                    part += fold(c, value)
                    acc[h, at] = jnp.zeros((KU, 128), jnp.float32)
                    if c in (1, 2):
                        send_own(q, h, c - 1)
                if h == 1:
                    send_own(q, 0, 2)
                    send_own(q, 1, 2)
                    for half in range(2):
                        wait_sends(p, half)
                        wait_mass_sends(p, half)
                    send_own(q, 0, 3)
                    send_own(q, 1, 3)
                send_mass(q, h, part)

            @pl.when(jnp.logical_not(more))
            def _():
                for c in range(4):
                    acc[h, pl.ds(c * KU, KU)] = next_rows(c)
                wait_sends(p, h)
                wait_mass_sends(p, h)

        return carry

    lax.fori_loop(0, num_sweeps, sweep, 0)


def finish(halves, out_hbm, sem):
    copies = [pltpu.make_async_copy(halves.at[h], out_hbm.at[:, pl.ds(h * 128, 128)], sem.at[h]) for h in range(2)]
    for copy in copies:
        copy.start()
    for copy in copies:
        copy.wait()


def solution(mesh):
    spec_rows = P(("batch", "row"), None)
    spec_vec = P(("batch", "row"))

    def local_sweeps(mat_rows, tele_rows, dang_rows, damping, start_rows):
        rows, nodes = mat_rows.shape
        seeds = start_rows.shape[1]
        num_sweeps = damping.shape[0]
        any_space = pl.BlockSpec(memory_space=pl.ANY)
        vmem = pl.BlockSpec(memory_space=pltpu.VMEM)
        sem = pltpu.SemaphoreType.DMA
        halves = pl.pallas_call(
            functools.partial(kernel, num_sweeps),
            out_shape=pltpu.VMEM((2, rows, 128), jnp.float32),
            in_specs=[any_space, any_space, any_space, pl.BlockSpec(memory_space=pltpu.SMEM), any_space],
            out_specs=vmem,
            scratch_shapes=[
                pltpu.VMEM((2, 2, 8, rows, 128), jnp.bfloat16),
                pltpu.VMEM((RING, rows, 2 * KU), jnp.bfloat16),
                pltpu.VMEM((2, 4, rows, KU), jnp.bfloat16),
                pltpu.VMEM((2, rows, 128), jnp.float32),
                pltpu.VMEM((rows, 128), jnp.float32),
                pltpu.VMEM((rows // 128, 128), jnp.int32),
                pltpu.VMEM((2, 2, 8, 1, 128), jnp.float32),
                sem((8, 2, 2, 4)),
                sem((8, 2, 2)),
                sem((2, 2, 8)),
                sem((2, 2)),
                sem((RING,)),
                sem((2, 4, 2)),
                sem((5,)),
                pltpu.SemaphoreType.REGULAR((2,)),
            ],
            compiler_params=pltpu.CompilerParams(collective_id=0, has_side_effects=True, vmem_limit_bytes=KERNEL_VMEM),
            name="sweeps",
        )(mat_rows, tele_rows, dang_rows.reshape(rows // 128, 128), damping, start_rows)
        return pl.pallas_call(
            finish,
            out_shape=jax.ShapeDtypeStruct((rows, seeds), jnp.float32),
            in_specs=[vmem],
            out_specs=any_space,
            scratch_shapes=[sem((2,))],
            compiler_params=pltpu.CompilerParams(vmem_limit_bytes=8 << 20),
            name="finish",
        )(halves)

    return jax.shard_map(local_sweeps, mesh=mesh, in_specs=(spec_rows, spec_rows, spec_vec, P(None), spec_rows),
                         out_specs=spec_rows, check_vma=False)
```

```python
import functools

import jax
import jax.numpy as jnp
from jax import lax
from jax.experimental import pallas as pl
from jax.experimental.pallas import tpu as pltpu
from jax.sharding import PartitionSpec as P

MESH = pl.DeviceIdType.MESH
OWN, SIB, XN, XS, YN, YS, DG, DS = range(8)
X_OWN, Y_OWN, X_FWD, Y_FWD, S_OWN, S_X, S_Y, S_D = range(8)
RING = 6
UNITS = 12
KU = 512
KF = 256
MB = 512
NEAR = (SIB, XN, YN)
KERNEL_VMEM = 64487424


def flip(a, b):
    return a + b - 2 * a * b


def kernel(num_sweeps, a_hbm, e_hbm, d_hbm, damp, r_hbm, acc, g, ring, res, ev, dcol, dbuf, mass,
           recv, send, mrecv, msend, ring_sem, res_sem, io_sem):
    rows = acc.shape[1]
    nodes = a_hbm.shape[1]
    group = lax.axis_index("batch")
    me = lax.axis_index("row")
    core = lax.rem(me, 2)
    xpos = lax.rem(lax.div(me, 2), 2)
    ypos = lax.div(me, 4)

    def index_of(slot):
        sbit, xbit, ybit = slot & 1, (slot >> 1) & 1, (slot >> 2) & 1
        return (flip(ypos, ybit) * 2 + flip(xpos, xbit)) * 2 + flip(core, sbit)

    def peer(slot):
        return (group, index_of(slot))

    barrier = pltpu.get_barrier_semaphore()
    for slot in NEAR:
        pl.semaphore_signal(barrier, inc=1, device_id=peer(slot), device_id_type=MESH)

    def remote(kind, p, h, c, src, dst):
        to = {X_OWN: XN, Y_OWN: YN, X_FWD: XN, Y_FWD: YN}.get(kind, SIB)
        return pltpu.make_async_remote_copy(src_ref=src, dst_ref=dst, send_sem=send.at[kind, p, h],
                                            recv_sem=recv.at[kind, p, h, c], device_id=peer(to), device_id_type=MESH)

    def block_copy(kind, p, h, c):
        src, dst = {X_OWN: (OWN, XN), Y_OWN: (OWN, YN), S_OWN: (OWN, SIB), S_X: (XN, XS), S_Y: (YN, YS),
                    S_D: (DG, DS)}[kind]
        at = pl.ds(pl.multiple_of(c * KU, KU), KU)
        return remote(kind, p, h, c, g.at[p, h, src, at], g.at[p, h, dst, at])

    def relay_copy(kind, p, h, f):
        src, start, part = (YN, 0, 0) if kind == X_FWD else (XN, rows // 2, KF)
        return remote(kind, p, h, f, g.at[p, h, src, pl.ds(start + f * KF, KF)],
                      g.at[p, h, DG, pl.ds(f * KU + part, KF)])

    def wait_relay(kind, p, h, f):
        part = 0 if kind == X_FWD else KF
        at = g.at[p, h, DG, pl.ds(pl.multiple_of(f * KU + part, KF), KF)]
        remote(kind, p, h, f, at, at).wait_recv()

    def wait_sends(p, h):
        for kind in range(8):
            size = rows // 2 if kind in (X_FWD, Y_FWD) else rows
            at = g.at[p, h, OWN, pl.ds(0, size)]
            remote(kind, p, h, 0, at, at).wait_send()

    def parts_of(u):
        if u < 4:
            return [(u // 2, 2 * (u % 2)), (u // 2, 2 * (u % 2) + 1)]
        return [(slot, (u - 4) // 2) for slot in ((XN, YN) if u % 2 == 0 else (XS, YS))]

    def start_unit(u):
        parts = parts_of(u)
        if parts[0][0] == parts[1][0]:
            parts = [(parts[0][0], parts[0][1], 0, 2 * KU)]
        else:
            parts = [(slot, c, i * KU, KU) for i, (slot, c) in enumerate(parts)]
        for slot, c, to, size in parts:
            col = pl.multiple_of(index_of(slot) * rows + c * KU, KU)
            pltpu.make_async_copy(a_hbm.at[:, pl.ds(col, size)], ring.at[u % RING, :, pl.ds(to, size)],
                                  ring_sem.at[u % RING]).start()

    def wait_unit(u):
        at = ring.at[u % RING]
        pltpu.make_async_copy(at, at, ring_sem.at[u % RING]).wait()

    def res_copy(i, f, part):
        col = pl.multiple_of(index_of(DG + i) * rows + f * KF + part * (rows // 2), KF)
        return pltpu.make_async_copy(a_hbm.at[:, pl.ds(col, KF)], res.at[i, f, :, pl.ds(part * KF, KF)],
                                     res_sem.at[i, f, part])

    def half_copy(src, dst, h, sem):
        return pltpu.make_async_copy(src.at[:, pl.ds(h * 128, 128)], dst.at[h], sem)

    for h in range(2):
        half_copy(r_hbm, acc, h, io_sem.at[h]).start()
    d_copy = pltpu.make_async_copy(d_hbm, dbuf, io_sem.at[4])
    d_copy.start()
    pl.semaphore_wait(barrier, 3)

    def send_own(p, h, c, kinds=(X_OWN, Y_OWN, S_OWN)):
        for kind in kinds:
            block_copy(kind, p, h, c).start()

    def mass_copy(p, i):
        return pltpu.make_async_remote_copy(src_ref=mass.at[p, i, 0], dst_ref=mass.at[p, i, 1],
                                            send_sem=msend.at[p, i], recv_sem=mrecv.at[p, i],
                                            device_id=peer(NEAR[i]), device_id_type=MESH)

    def take_mass(p, i):
        mass_copy(p, i).wait_recv()
        mass[p, i + 1, 0] = mass[p, i, 0] + mass[p, i, 1]

    def fold(c, value):
        weighed = value * dcol[pl.ds(c * KU, KU), :]
        return jnp.sum(weighed.reshape(KU // 8, 8, 128), axis=0)

    for h in range(2):
        half_copy(r_hbm, acc, h, io_sem.at[h]).wait()
        for c in range(4):
            at = pl.ds(c * KU, KU)
            g[0, h, OWN, at] = acc[h, at].astype(jnp.bfloat16)
            if h == 0 and c in (1, 2):
                send_own(0, 0, c - 1)
    for h, c in ((1, 0), (1, 1)):
        send_own(0, h, c)
    for h, c in ((0, 2), (1, 2), (0, 3), (1, 3)):
        send_own(0, h, c, (S_OWN,))

    for u in range(RING):
        start_unit(u)
    for h in range(2):
        half_copy(e_hbm, ev, h, io_sem.at[2 + h]).start()
    for i in range(2):
        for f in range(4):
            for part in range(2):
                res_copy(i, f, part).start()
    d_copy.wait()
    for c in range(rows // 128):
        line = jnp.broadcast_to(dbuf[pl.ds(c, 1), :].astype(jnp.float32), (128, 128))
        dcol[pl.ds(c * 128, 128), :] = line.T
    for h in range(2):
        part = jnp.zeros((8, 128), jnp.float32)
        for c in range(4):
            part += fold(c, acc[h, pl.ds(c * KU, KU)])
        mass[0, 0, 0, :, h * 128:(h + 1) * 128] = jnp.sum(part, axis=0, keepdims=True)
        acc[h] = jnp.zeros_like(acc[h])
    mass_copy(0, 0).start()

    def sweep(t, carry):
        p = lax.rem(t, 2)
        q = 1 - p
        more = t < num_sweeps - 1
        factor = damp[t]

        def wide(u):
            wait_unit(u)
            piece = jnp.concatenate(
                [jnp.concatenate([g[p, h, slot, pl.ds(c * KU, KU)] for h in range(2)], axis=1) for slot, c in parts_of(u)],
                axis=0)
            for m in range(rows // MB):
                mt = pl.ds(m * MB, MB)
                prod = jnp.dot(ring[u % RING, mt], piece, preferred_element_type=jnp.float32)
                acc[0, mt] += prod[:, :128]
                acc[1, mt] += prod[:, 128:]
            if u + RING < UNITS:
                start_unit(u + RING)
            else:
                @pl.when(more)
                def _():
                    start_unit(u + RING - UNITS)

        wide(0)
        take_mass(p, 0)
        for h in range(2):
            send_own(p, h, 2, (Y_OWN,))
        mass_copy(p, 1).start()
        for h, c, kind in ((0, 2, X_OWN), (1, 2, X_OWN), (0, 3, X_OWN), (0, 3, Y_OWN), (1, 3, X_OWN), (1, 3, Y_OWN)):
            send_own(p, h, c, (kind,))
        wide(1)
        for u in (2, 3):
            for slot, c in parts_of(u):
                for h in range(2):
                    block_copy(S_OWN, p, h, c).wait_recv()
            wide(u)
        for c in range(4):
            for h in range(2):
                block_copy(X_OWN, p, h, c).wait_recv()
                block_copy(S_X, p, h, c).start()
                block_copy(Y_OWN, p, h, c).wait_recv()
                block_copy(S_Y, p, h, c).start()
                kind = X_FWD if c < 2 else Y_FWD
                here = (2 * (c % 2), 2 * (c % 2) + 1)

                @pl.when(more)
                def _():
                    for f in here if h == 0 else range(4 * (c % 2)):
                        relay_copy(kind, p, h, f).start()

                @pl.when(jnp.logical_not(more))
                def _():
                    for f in here if h == 1 else ():
                        relay_copy(kind, p, 0, f).start()
                        relay_copy(kind, p, 1, f).start()
            if c == 1:
                take_mass(p, 1)
            wide(2 * c + 4)
            if c == 1:
                mass_copy(p, 2).start()
            for h in range(2):
                block_copy(S_X, p, h, c).wait_recv()
                block_copy(S_Y, p, h, c).wait_recv()
            wide(2 * c + 5)

        @pl.when(t == 0)
        def _():
            for h in range(2):
                half_copy(e_hbm, ev, h, io_sem.at[2 + h]).wait()
            for i in range(2):
                for f in range(4):
                    for part in range(2):
                        res_copy(i, f, part).wait()

        take_mass(p, 2)

        def take(h, f):
            wait_relay(X_FWD, p, h, f)
            wait_relay(Y_FWD, p, h, f)
            block_copy(S_D, p, h, f).start()

        def right(h, i, f):
            return g[p, h, DG + i, pl.ds(pl.multiple_of(f * KU, KU), KU)]

        def next_rows(h, c):
            at = pl.ds(c * KU, KU)
            line = (factor / nodes) * mass[p, 3, 0, :, h * 128:(h + 1) * 128]
            return factor * acc[h, at] + (1.0 - factor) * ev[h, at] + line

        def wait_all_sends():
            for h in range(2):
                wait_sends(p, h)
            for i in range(3):
                mass_copy(p, i).wait_send()

        @pl.when(more)
        def _():
            for h in range(2):
                def narrow(*terms):
                    pieces = [right(h, i, f) for i, f in terms]
                    piece = jnp.concatenate(pieces, axis=0) if len(terms) > 1 else pieces[0]
                    for m in range(rows // MB):
                        mt = pl.ds(m * MB, MB)
                        left = [res[i, f, mt] for i, f in terms]
                        left = jnp.concatenate(left, axis=1) if len(terms) > 1 else left[0]
                        acc[h, mt] += jnp.dot(left, piece, preferred_element_type=jnp.float32)

                take(h, 0)
                narrow((0, 0))

                @pl.loop(1, 4)
                def _(f):
                    take(h, f)
                    block_copy(S_D, p, h, f - 1).wait_recv()
                    narrow((0, f), (1, f - 1))

                block_copy(S_D, p, h, 3).wait_recv()
                narrow((1, 3))

                part = jnp.zeros((8, 128), jnp.float32)
                for c in range(4):
                    at = pl.ds(c * KU, KU)
                    value = next_rows(h, c)
                    g[q, h, OWN, at] = value.astype(jnp.bfloat16)
                    part += fold(c, value)
                    acc[h, at] = jnp.zeros((KU, 128), jnp.float32)
                    if c in (1, 2):
                        send_own(q, h, c - 1)
                mass[q, 0, 0, :, h * 128:(h + 1) * 128] = jnp.sum(part, axis=0, keepdims=True)
            for h in range(2):
                send_own(q, h, 2, (S_OWN,))
            mass_copy(q, 0).start()
            wait_all_sends()
            for h in range(2):
                send_own(q, h, 3, (S_OWN,))

        @pl.when(jnp.logical_not(more))
        def _():
            def both(i, f):
                piece = jnp.concatenate([right(h, i, f) for h in range(2)], axis=1)
                for m in range(rows // MB):
                    mt = pl.ds(m * MB, MB)
                    prod = jnp.dot(res[i, f, mt], piece, preferred_element_type=jnp.float32)
                    acc[0, mt] += prod[:, :128]
                    acc[1, mt] += prod[:, 128:]

            @pl.loop(0, 4)
            def _(f):
                for h in range(2):
                    take(h, f)
                both(0, f)
                for h in range(2):
                    block_copy(S_D, p, h, f).wait_recv()
                both(1, f)

            for h in range(2):
                for c in range(4):
                    acc[h, pl.ds(c * KU, KU)] = next_rows(h, c)
            wait_all_sends()

        return carry

    lax.fori_loop(0, num_sweeps, sweep, 0)


def finish(halves, out_hbm, sem):
    copies = [pltpu.make_async_copy(halves.at[h], out_hbm.at[:, pl.ds(h * 128, 128)], sem.at[h]) for h in range(2)]
    for copy in copies:
        copy.start()
    for copy in copies:
        copy.wait()


def solution(mesh):
    spec_rows = P(("batch", "row"), None)
    spec_vec = P(("batch", "row"))

    def local_sweeps(mat_rows, tele_rows, dang_rows, damping, start_rows):
        rows, nodes = mat_rows.shape
        seeds = start_rows.shape[1]
        num_sweeps = damping.shape[0]
        any_space = pl.BlockSpec(memory_space=pl.ANY)
        vmem = pl.BlockSpec(memory_space=pltpu.VMEM)
        sem = pltpu.SemaphoreType.DMA
        halves = pl.pallas_call(
            functools.partial(kernel, num_sweeps),
            out_shape=pltpu.VMEM((2, rows, 128), jnp.float32),
            in_specs=[any_space, any_space, any_space, pl.BlockSpec(memory_space=pltpu.SMEM), any_space],
            out_specs=vmem,
            scratch_shapes=[
                pltpu.VMEM((2, 2, 8, rows, 128), jnp.bfloat16),
                pltpu.VMEM((RING, rows, 2 * KU), jnp.bfloat16),
                pltpu.VMEM((2, 4, rows, KU), jnp.bfloat16),
                pltpu.VMEM((2, rows, 128), jnp.float32),
                pltpu.VMEM((rows, 128), jnp.float32),
                pltpu.VMEM((rows // 128, 128), jnp.int32),
                pltpu.VMEM((2, 4, 2, 1, 256), jnp.float32),
                sem((8, 2, 2, 4)),
                sem((8, 2, 2)),
                sem((2, 3)),
                sem((2, 3)),
                sem((RING,)),
                sem((2, 4, 2)),
                sem((5,)),
            ],
            compiler_params=pltpu.CompilerParams(collective_id=0, has_side_effects=True, vmem_limit_bytes=KERNEL_VMEM),
            name="sweeps",
        )(mat_rows, tele_rows, dang_rows.reshape(rows // 128, 128), damping, start_rows)
        return pl.pallas_call(
            finish,
            out_shape=jax.ShapeDtypeStruct((rows, seeds), jnp.float32),
            in_specs=[vmem],
            out_specs=any_space,
            scratch_shapes=[sem((2,))],
            compiler_params=pltpu.CompilerParams(vmem_limit_bytes=8 << 20),
            name="finish",
        )(halves)

    return jax.shard_map(local_sweeps, mesh=mesh, in_specs=(spec_rows, spec_rows, spec_vec, P(None), spec_rows),
                         out_specs=spec_rows, check_vma=False)
```

```python
import functools

import jax
import jax.numpy as jnp
from jax import lax
from jax.experimental import pallas as pl
from jax.experimental.pallas import tpu as pltpu
from jax.sharding import PartitionSpec as P

MESH = pl.DeviceIdType.MESH
OWN, SIB, XN, XS, YN, YS, DG, DS = range(8)
X_OWN, Y_OWN, X_FWD, Y_FWD, S_OWN, S_X, S_Y, S_D = range(8)
RING = 6
UNITS = 12
KU = 512
KF = 256
MB = 512
NEAR = (SIB, XN, YN)
KERNEL_VMEM = 64487424


def flip(a, b):
    return a + b - 2 * a * b


def kernel(num_sweeps, a_hbm, e_hbm, d_hbm, damp, r_hbm, acc, g, ring, res, ev, dcol, dbuf, mass,
           near_sem, relay_sem, sib_sem, pass_sem, far_sem, send, mrecv, msend, ring_sem, res_sem, io_sem):
    rows = acc.shape[1]
    nodes = a_hbm.shape[1]
    group = lax.axis_index("batch")
    me = lax.axis_index("row")
    core = lax.rem(me, 2)
    xpos = lax.rem(lax.div(me, 2), 2)
    ypos = lax.div(me, 4)

    def index_of(slot):
        sbit, xbit, ybit = slot & 1, (slot >> 1) & 1, (slot >> 2) & 1
        return (flip(ypos, ybit) * 2 + flip(xpos, xbit)) * 2 + flip(core, sbit)

    def peer(slot):
        return (group, index_of(slot))

    barrier = pltpu.get_barrier_semaphore()
    for slot in NEAR:
        pl.semaphore_signal(barrier, inc=1, device_id=peer(slot), device_id_type=MESH)

    def arrival(kind, p, h, c):
        if kind in (X_OWN, Y_OWN):
            return near_sem.at[p, h, c]
        if kind in (X_FWD, Y_FWD):
            return relay_sem.at[h, c]
        if kind == S_OWN:
            return sib_sem.at[c // 2]
        return far_sem.at[h, c] if kind == S_D else pass_sem.at[c]

    def remote(kind, p, h, c, src, dst):
        to = {X_OWN: XN, Y_OWN: YN, X_FWD: XN, Y_FWD: YN}.get(kind, SIB)
        return pltpu.make_async_remote_copy(src_ref=src, dst_ref=dst, send_sem=send.at[p, h],
                                            recv_sem=arrival(kind, p, h, c), device_id=peer(to), device_id_type=MESH)

    def block_copy(kind, p, h, c):
        src, dst = {X_OWN: (OWN, XN), Y_OWN: (OWN, YN), S_OWN: (OWN, SIB), S_X: (XN, XS), S_Y: (YN, YS),
                    S_D: (DG, DS)}[kind]
        at = pl.ds(pl.multiple_of(c * KU, KU), KU)
        return remote(kind, p, h, c, g.at[p, h, src, at], g.at[p, h, dst, at])

    def relay_copy(kind, p, h, f):
        src, start, part = (YN, 0, 0) if kind == X_FWD else (XN, rows // 2, KF)
        return remote(kind, p, h, f, g.at[p, h, src, pl.ds(start + f * KF, KF)],
                      g.at[p, h, DG, pl.ds(f * KU + part, KF)])

    def wait_near(p, h, c):
        at = g.at[p, h, pl.ds(0, 2), pl.ds(c * KU, KU)]
        remote(X_OWN, p, h, c, at, at).wait_recv()

    def wait_relays(p, h, f):
        at = g.at[p, h, DG, pl.ds(pl.multiple_of(f * KU, KU), KU)]
        remote(X_FWD, p, h, f, at, at).wait_recv()

    def wait_sib(p, half):
        at = g.at[p, :, SIB, pl.ds(half * 2 * KU, 2 * KU)]
        remote(S_OWN, p, 0, 2 * half, at, at).wait_recv()

    def wait_passed(p, c):
        at = g.at[p, :, pl.ds(0, 2), pl.ds(c * KU, KU)]
        remote(S_X, p, 0, c, at, at).wait_recv()

    def wait_sends(p, h):
        at = g.at[p, h, pl.ds(0, 7)]
        remote(S_D, p, h, 0, at, at).wait_send()

    def parts_of(u):
        if u < 4:
            return [(u // 2, 2 * (u % 2)), (u // 2, 2 * (u % 2) + 1)]
        return [(slot, (u - 4) // 2) for slot in ((XN, YN) if u % 2 == 0 else (XS, YS))]

    def start_unit(u):
        parts = parts_of(u)
        if parts[0][0] == parts[1][0]:
            parts = [(parts[0][0], parts[0][1], 0, 2 * KU)]
        else:
            parts = [(slot, c, i * KU, KU) for i, (slot, c) in enumerate(parts)]
        for slot, c, to, size in parts:
            col = pl.multiple_of(index_of(slot) * rows + c * KU, KU)
            pltpu.make_async_copy(a_hbm.at[:, pl.ds(col, size)], ring.at[u % RING, :, pl.ds(to, size)],
                                  ring_sem.at[u % RING]).start()

    def wait_unit(u):
        at = ring.at[u % RING]
        pltpu.make_async_copy(at, at, ring_sem.at[u % RING]).wait()

    def res_copy(i, f, part):
        col = pl.multiple_of(index_of(DG + i) * rows + f * KF + part * (rows // 2), KF)
        return pltpu.make_async_copy(a_hbm.at[:, pl.ds(col, KF)], res.at[i, f, :, pl.ds(part * KF, KF)],
                                     res_sem.at[i, f // 2])

    def half_copy(src, dst, h, sem):
        return pltpu.make_async_copy(src.at[:, pl.ds(h * 128, 128)], dst.at[h], sem)

    for h in range(2):
        half_copy(r_hbm, acc, h, io_sem.at[h]).start()
    d_copy = pltpu.make_async_copy(d_hbm, dbuf, io_sem.at[3])
    d_copy.start()
    pl.semaphore_wait(barrier, 3)

    def send_own(p, h, c, kinds=(X_OWN, Y_OWN, S_OWN)):
        for kind in kinds:
            block_copy(kind, p, h, c).start()

    def mass_copy(p, i):
        return pltpu.make_async_remote_copy(src_ref=mass.at[p, i, 0], dst_ref=mass.at[p, i, 1],
                                            send_sem=msend.at[p], recv_sem=mrecv.at[p, i],
                                            device_id=peer(NEAR[i]), device_id_type=MESH)

    def take_mass(p, i):
        mass_copy(p, i).wait_recv()
        mass[p, i + 1, 0] = mass[p, i, 0] + mass[p, i, 1]

    def fold(c, value):
        weighed = value * dcol[pl.ds(c * KU, KU), :]
        return jnp.sum(weighed.reshape(KU // 8, 8, 128), axis=0)

    for h in range(2):
        half_copy(r_hbm, acc, h, io_sem.at[h]).wait()
        for c in range(4):
            at = pl.ds(c * KU, KU)
            g[0, h, OWN, at] = acc[h, at].astype(jnp.bfloat16)
            if h == 0 and c in (1, 2):
                send_own(0, 0, c - 1)
    for h, c in ((1, 0), (1, 1)):
        send_own(0, h, c)
    for h, c in ((0, 2), (1, 2), (0, 3), (1, 3)):
        send_own(0, h, c, (S_OWN,))

    for u in range(RING):
        start_unit(u)
    for h in range(2):
        half_copy(e_hbm, ev, h, io_sem.at[2]).start()
    for i in range(2):
        for f in range(4):
            for part in range(2):
                res_copy(i, f, part).start()
    d_copy.wait()
    for c in range(rows // 128):
        line = jnp.broadcast_to(dbuf[pl.ds(c, 1), :].astype(jnp.float32), (128, 128))
        dcol[pl.ds(c * 128, 128), :] = line.T
    for h in range(2):
        part = jnp.zeros((8, 128), jnp.float32)
        for c in range(4):
            part += fold(c, acc[h, pl.ds(c * KU, KU)])
        mass[0, 0, 0, :, h * 128:(h + 1) * 128] = jnp.sum(part, axis=0, keepdims=True)
        acc[h] = jnp.zeros_like(acc[h])
    mass_copy(0, 0).start()

    def sweep(t, carry):
        p = lax.rem(t, 2)
        q = 1 - p
        more = t < num_sweeps - 1
        factor = damp[t]

        def wide(u):
            wait_unit(u)
            piece = jnp.concatenate(
                [jnp.concatenate([g[p, h, slot, pl.ds(c * KU, KU)] for h in range(2)], axis=1) for slot, c in parts_of(u)],
                axis=0)
            for m in range(rows // MB):
                mt = pl.ds(m * MB, MB)
                prod = jnp.dot(ring[u % RING, mt], piece, preferred_element_type=jnp.float32)
                acc[0, mt] += prod[:, :128]
                acc[1, mt] += prod[:, 128:]
            if u + RING < UNITS:
                start_unit(u + RING)
            else:
                @pl.when(more)
                def _():
                    start_unit(u + RING - UNITS)

        wide(0)
        take_mass(p, 0)
        for h in range(2):
            send_own(p, h, 2, (Y_OWN,))
        mass_copy(p, 1).start()
        for h, c, kind in ((0, 2, X_OWN), (1, 2, X_OWN), (0, 3, X_OWN), (0, 3, Y_OWN), (1, 3, X_OWN), (1, 3, Y_OWN)):
            send_own(p, h, c, (kind,))
        wide(1)
        for u in (2, 3):
            wait_sib(p, u - 2)
            wide(u)
        for c in range(4):
            for h in range(2):
                wait_near(p, h, c)
                block_copy(S_X, p, h, c).start()
                block_copy(S_Y, p, h, c).start()
                kind = X_FWD if c < 2 else Y_FWD
                here = (2 * (c % 2), 2 * (c % 2) + 1)

                @pl.when(more)
                def _():
                    for f in here if h == 0 else range(4 * (c % 2)):
                        relay_copy(kind, p, h, f).start()

                @pl.when(jnp.logical_not(more))
                def _():
                    for f in here if h == 1 else ():
                        relay_copy(kind, p, 0, f).start()
                        relay_copy(kind, p, 1, f).start()
            if c == 1:
                take_mass(p, 1)
            wide(2 * c + 4)
            if c == 1:
                mass_copy(p, 2).start()
            wait_passed(p, c)
            wide(2 * c + 5)

        @pl.when(t == 0)
        def _():
            pltpu.make_async_copy(ev, ev, io_sem.at[2]).wait()
            for i in range(2):
                for half in range(2):
                    at = res.at[i, pl.ds(2 * half, 2)]
                    pltpu.make_async_copy(at, at, res_sem.at[i, half]).wait()

        take_mass(p, 2)

        def take(h, f):
            wait_relays(p, h, f)
            block_copy(S_D, p, h, f).start()

        def right(h, i, f):
            return g[p, h, DG + i, pl.ds(pl.multiple_of(f * KU, KU), KU)]

        def next_rows(h, c):
            at = pl.ds(c * KU, KU)
            line = (factor / nodes) * mass[p, 3, 0, :, h * 128:(h + 1) * 128]
            return factor * acc[h, at] + (1.0 - factor) * ev[h, at] + line

        def wait_all_sends():
            for h in range(2):
                wait_sends(p, h)
            at = mass.at[p, pl.ds(0, 3), 0]
            pltpu.make_async_remote_copy(src_ref=at, dst_ref=at, send_sem=msend.at[p], recv_sem=mrecv.at[p, 0],
                                         device_id=peer(SIB), device_id_type=MESH).wait_send()

        @pl.when(more)
        def _():
            for h in range(2):
                def narrow(*terms):
                    pieces = [right(h, i, f) for i, f in terms]
                    piece = jnp.concatenate(pieces, axis=0) if len(terms) > 1 else pieces[0]
                    for m in range(rows // MB):
                        mt = pl.ds(m * MB, MB)
                        left = [res[i, f, mt] for i, f in terms]
                        left = jnp.concatenate(left, axis=1) if len(terms) > 1 else left[0]
                        acc[h, mt] += jnp.dot(left, piece, preferred_element_type=jnp.float32)

                take(h, 0)
                narrow((0, 0))

                @pl.loop(1, 4)
                def _(f):
                    take(h, f)
                    block_copy(S_D, p, h, f - 1).wait_recv()
                    narrow((0, f), (1, f - 1))

                block_copy(S_D, p, h, 3).wait_recv()
                narrow((1, 3))

                part = jnp.zeros((8, 128), jnp.float32)
                for c in range(4):
                    at = pl.ds(c * KU, KU)
                    value = next_rows(h, c)
                    g[q, h, OWN, at] = value.astype(jnp.bfloat16)
                    part += fold(c, value)
                    acc[h, at] = jnp.zeros((KU, 128), jnp.float32)
                    if c in (1, 2):
                        send_own(q, h, c - 1)
                mass[q, 0, 0, :, h * 128:(h + 1) * 128] = jnp.sum(part, axis=0, keepdims=True)
            for h in range(2):
                send_own(q, h, 2, (S_OWN,))
            mass_copy(q, 0).start()
            wait_all_sends()
            for h in range(2):
                send_own(q, h, 3, (S_OWN,))

        @pl.when(jnp.logical_not(more))
        def _():
            def both(i, f, scale=None):
                piece = jnp.concatenate([right(h, i, f) for h in range(2)], axis=1)
                for m in range(rows // MB):
                    mt = pl.ds(m * MB, MB)
                    prod = jnp.dot(res[i, f, mt], piece, preferred_element_type=jnp.float32)
                    if scale is not None:
                        prod = scale * prod
                    acc[0, mt] += prod[:, :128]
                    acc[1, mt] += prod[:, 128:]

            def take_both(f):
                for h in range(2):
                    take(h, f)

            def wait_far(f):
                for h in range(2):
                    block_copy(S_D, p, h, f).wait_recv()

            @pl.loop(0, 3)
            def _(f):
                take_both(f)
                both(0, f)
                wait_far(f)
                both(1, f)

            for h in range(2):
                for c in range(4):
                    acc[h, pl.ds(c * KU, KU)] = next_rows(h, c)
            take_both(3)
            both(0, 3, factor)
            wait_far(3)
            both(1, 3, factor)
            wait_all_sends()

        return carry

    lax.fori_loop(0, num_sweeps, sweep, 0)


def finish(halves, out_hbm, sem):
    copies = [pltpu.make_async_copy(halves.at[h], out_hbm.at[:, pl.ds(h * 128, 128)], sem.at[h]) for h in range(2)]
    for copy in copies:
        copy.start()
    for copy in copies:
        copy.wait()


def solution(mesh):
    spec_rows = P(("batch", "row"), None)
    spec_vec = P(("batch", "row"))

    def local_sweeps(mat_rows, tele_rows, dang_rows, damping, start_rows):
        rows, nodes = mat_rows.shape
        seeds = start_rows.shape[1]
        num_sweeps = damping.shape[0]
        any_space = pl.BlockSpec(memory_space=pl.ANY)
        vmem = pl.BlockSpec(memory_space=pltpu.VMEM)
        sem = pltpu.SemaphoreType.DMA
        halves = pl.pallas_call(
            functools.partial(kernel, num_sweeps),
            out_shape=pltpu.VMEM((2, rows, 128), jnp.float32),
            in_specs=[any_space, any_space, any_space, pl.BlockSpec(memory_space=pltpu.SMEM), any_space],
            out_specs=vmem,
            scratch_shapes=[
                pltpu.VMEM((2, 2, 8, rows, 128), jnp.bfloat16),
                pltpu.VMEM((RING, rows, 2 * KU), jnp.bfloat16),
                pltpu.VMEM((2, 4, rows, KU), jnp.bfloat16),
                pltpu.VMEM((2, rows, 128), jnp.float32),
                pltpu.VMEM((rows, 128), jnp.float32),
                pltpu.VMEM((rows // 128, 128), jnp.int32),
                pltpu.VMEM((2, 4, 2, 1, 256), jnp.float32),
                sem((2, 2, 4)),
                sem((2, 4)),
                sem((2,)),
                sem((4,)),
                sem((2, 4)),
                sem((2, 2)),
                sem((2, 3)),
                sem((2,)),
                sem((RING,)),
                sem((2, 2)),
                sem((4,)),
            ],
            compiler_params=pltpu.CompilerParams(collective_id=0, has_side_effects=True, vmem_limit_bytes=KERNEL_VMEM),
            name="sweeps",
        )(mat_rows, tele_rows, dang_rows.reshape(rows // 128, 128), damping, start_rows)
        return pl.pallas_call(
            finish,
            out_shape=jax.ShapeDtypeStruct((rows, seeds), jnp.float32),
            in_specs=[vmem],
            out_specs=any_space,
            scratch_shapes=[sem((2,))],
            compiler_params=pltpu.CompilerParams(vmem_limit_bytes=8 << 20),
            name="finish",
        )(halves)

    return jax.shard_map(local_sweeps, mesh=mesh, in_specs=(spec_rows, spec_rows, spec_vec, P(None), spec_rows),
                         out_specs=spec_rows, check_vma=False)
```

```python
import functools

import jax
import jax.numpy as jnp
from jax import lax
from jax.experimental import pallas as pl
from jax.experimental.pallas import tpu as pltpu
from jax.sharding import PartitionSpec as P

MESH = pl.DeviceIdType.MESH
OWN, SIB, XN, XS, YN, YS, DG, DS = range(8)
X_OWN, Y_OWN, X_FWD, Y_FWD, S_OWN, S_X, S_Y, S_D = range(8)
RING = 6
UNITS = 12
KU = 512
KF = 256
MB = 512
NEAR = (SIB, XN, YN)
KERNEL_VMEM = 64487424


def flip(a, b):
    return a + b - 2 * a * b


def kernel(num_sweeps, a_hbm, e_hbm, d_hbm, damp_hbm, r_hbm, acc, g, ring, res, ev, dcol, dbuf, damp, mass,
           near_sem, relay_sem, sib_sem, pass_sem, far_sem, send, mrecv, msend, ring_sem, res_sem, io_sem):
    rows = acc.shape[1]
    nodes = a_hbm.shape[1]
    group = lax.axis_index("batch")
    me = lax.axis_index("row")
    core = lax.rem(me, 2)
    xpos = lax.rem(lax.div(me, 2), 2)
    ypos = lax.div(me, 4)

    def index_of(slot):
        sbit, xbit, ybit = slot & 1, (slot >> 1) & 1, (slot >> 2) & 1
        return (flip(ypos, ybit) * 2 + flip(xpos, xbit)) * 2 + flip(core, sbit)

    def peer(slot):
        return (group, index_of(slot))

    barrier = pltpu.get_barrier_semaphore()
    for slot in NEAR:
        pl.semaphore_signal(barrier, inc=1, device_id=peer(slot), device_id_type=MESH)

    def arrival(kind, p, h, c):
        if kind in (X_OWN, Y_OWN):
            return near_sem.at[p, h, c]
        if kind in (X_FWD, Y_FWD):
            return relay_sem.at[h, c]
        if kind == S_OWN:
            return sib_sem.at[c // 2]
        return far_sem.at[h, c] if kind == S_D else pass_sem.at[c]

    def remote(kind, p, h, c, src, dst):
        to = {X_OWN: XN, Y_OWN: YN, X_FWD: XN, Y_FWD: YN}.get(kind, SIB)
        return pltpu.make_async_remote_copy(src_ref=src, dst_ref=dst, send_sem=send.at[p, h],
                                            recv_sem=arrival(kind, p, h, c), device_id=peer(to), device_id_type=MESH)

    def block_copy(kind, p, h, c):
        src, dst = {X_OWN: (OWN, XN), Y_OWN: (OWN, YN), S_OWN: (OWN, SIB), S_X: (XN, XS), S_Y: (YN, YS),
                    S_D: (DG, DS)}[kind]
        at = pl.ds(pl.multiple_of(c * KU, KU), KU)
        return remote(kind, p, h, c, g.at[p, h, src, at], g.at[p, h, dst, at])

    def relay_copy(kind, p, h, f):
        src, start, part = (YN, 0, 0) if kind == X_FWD else (XN, rows // 2, KF)
        return remote(kind, p, h, f, g.at[p, h, src, pl.ds(start + f * KF, KF)],
                      g.at[p, h, DG, pl.ds(f * KU + part, KF)])

    def wait_near(p, h, c):
        at = g.at[p, h, pl.ds(0, 2), pl.ds(c * KU, KU)]
        remote(X_OWN, p, h, c, at, at).wait_recv()

    def wait_relays(p, h, f):
        at = g.at[p, h, DG, pl.ds(pl.multiple_of(f * KU, KU), KU)]
        remote(X_FWD, p, h, f, at, at).wait_recv()

    def wait_sib(p, half):
        at = g.at[p, :, SIB, pl.ds(half * 2 * KU, 2 * KU)]
        remote(S_OWN, p, 0, 2 * half, at, at).wait_recv()

    def wait_passed(p, c):
        at = g.at[p, :, pl.ds(0, 2), pl.ds(c * KU, KU)]
        remote(S_X, p, 0, c, at, at).wait_recv()

    def wait_sends(p, h):
        at = g.at[p, h, pl.ds(0, 7)]
        remote(S_D, p, h, 0, at, at).wait_send()

    def parts_of(u):
        if u < 4:
            return [(u // 2, 2 * (u % 2)), (u // 2, 2 * (u % 2) + 1)]
        return [(slot, (u - 4) // 2) for slot in ((XN, YN) if u % 2 == 0 else (XS, YS))]

    def start_unit(u):
        parts = parts_of(u)
        if parts[0][0] == parts[1][0]:
            parts = [(parts[0][0], parts[0][1], 0, 2 * KU)]
        else:
            parts = [(slot, c, i * KU, KU) for i, (slot, c) in enumerate(parts)]
        for slot, c, to, size in parts:
            col = pl.multiple_of(index_of(slot) * rows + c * KU, KU)
            pltpu.make_async_copy(a_hbm.at[:, pl.ds(col, size)], ring.at[u % RING, :, pl.ds(to, size)],
                                  ring_sem.at[u % RING]).start()

    def wait_unit(u):
        at = ring.at[u % RING]
        pltpu.make_async_copy(at, at, ring_sem.at[u % RING]).wait()

    def res_copy(i, f, part):
        col = pl.multiple_of(index_of(DG + i) * rows + f * KF + part * (rows // 2), KF)
        return pltpu.make_async_copy(a_hbm.at[:, pl.ds(col, KF)], res.at[i, f, :, pl.ds(part * KF, KF)],
                                     res_sem.at[i, f // 2])

    def half_copy(src, dst, h, sem):
        return pltpu.make_async_copy(src.at[:, pl.ds(h * 128, 128)], dst.at[h], sem)

    for h in range(2):
        half_copy(r_hbm, acc, h, io_sem.at[h]).start()
    d_copy = pltpu.make_async_copy(d_hbm, dbuf, io_sem.at[3])
    d_copy.start()
    damp_copy = pltpu.make_async_copy(damp_hbm, damp, io_sem.at[4])
    damp_copy.start()
    pl.semaphore_wait(barrier, 3)

    def send_own(p, h, c, kinds=(X_OWN, Y_OWN, S_OWN)):
        for kind in kinds:
            block_copy(kind, p, h, c).start()

    def mass_copy(p, i):
        return pltpu.make_async_remote_copy(src_ref=mass.at[p, i, 0], dst_ref=mass.at[p, i, 1],
                                            send_sem=msend.at[p], recv_sem=mrecv.at[p, i],
                                            device_id=peer(NEAR[i]), device_id_type=MESH)

    def take_mass(p, i):
        mass_copy(p, i).wait_recv()
        mass[p, i + 1, 0] = mass[p, i, 0] + mass[p, i, 1]

    def fold(c, value):
        weighed = value * dcol[pl.ds(c * KU, KU), :]
        return jnp.sum(weighed.reshape(KU // 8, 8, 128), axis=0)

    for h in range(2):
        half_copy(r_hbm, acc, h, io_sem.at[h]).wait()
        for c in range(4):
            at = pl.ds(c * KU, KU)
            g[0, h, OWN, at] = acc[h, at].astype(jnp.bfloat16)
            if h == 0 and c in (1, 2):
                send_own(0, 0, c - 1)
    for h, c in ((1, 0), (1, 1)):
        send_own(0, h, c)
    for h, c in ((0, 2), (1, 2), (0, 3), (1, 3)):
        send_own(0, h, c, (S_OWN,))

    for u in range(RING):
        start_unit(u)
    for h in range(2):
        half_copy(e_hbm, ev, h, io_sem.at[2]).start()
    for i in range(2):
        for f in range(4):
            for part in range(2):
                res_copy(i, f, part).start()
    d_copy.wait()
    for c in range(rows // 128):
        line = jnp.broadcast_to(dbuf[pl.ds(c, 1), :].astype(jnp.float32), (128, 128))
        dcol[pl.ds(c * 128, 128), :] = line.T
    for h in range(2):
        part = jnp.zeros((8, 128), jnp.float32)
        for c in range(4):
            part += fold(c, acc[h, pl.ds(c * KU, KU)])
        mass[0, 0, 0, :, h * 128:(h + 1) * 128] = jnp.sum(part, axis=0, keepdims=True)
        acc[h] = jnp.zeros_like(acc[h])
    mass_copy(0, 0).start()
    damp_copy.wait()

    def sweep(t, carry):
        p = lax.rem(t, 2)
        q = 1 - p
        more = t < num_sweeps - 1
        factor = damp[t]

        def wide(u):
            wait_unit(u)
            piece = jnp.concatenate(
                [jnp.concatenate([g[p, h, slot, pl.ds(c * KU, KU)] for h in range(2)], axis=1) for slot, c in parts_of(u)],
                axis=0)
            for m in range(rows // MB):
                mt = pl.ds(m * MB, MB)
                prod = jnp.dot(ring[u % RING, mt], piece, preferred_element_type=jnp.float32)
                acc[0, mt] += prod[:, :128]
                acc[1, mt] += prod[:, 128:]
            if u + RING < UNITS:
                start_unit(u + RING)
            else:
                @pl.when(more)
                def _():
                    start_unit(u + RING - UNITS)

        wide(0)
        take_mass(p, 0)
        for h in range(2):
            send_own(p, h, 2, (Y_OWN,))
        mass_copy(p, 1).start()
        for h, c, kind in ((0, 2, X_OWN), (1, 2, X_OWN), (0, 3, X_OWN), (0, 3, Y_OWN), (1, 3, X_OWN), (1, 3, Y_OWN)):
            send_own(p, h, c, (kind,))
        wide(1)
        for u in (2, 3):
            wait_sib(p, u - 2)
            wide(u)
        for c in range(4):
            for h in range(2):
                wait_near(p, h, c)
                block_copy(S_X, p, h, c).start()
                block_copy(S_Y, p, h, c).start()
                kind = X_FWD if c < 2 else Y_FWD
                here = (2 * (c % 2), 2 * (c % 2) + 1)

                @pl.when(more)
                def _():
                    for f in here if h == 0 else range(4 * (c % 2)):
                        relay_copy(kind, p, h, f).start()

                @pl.when(jnp.logical_not(more))
                def _():
                    for f in here if h == 1 else ():
                        relay_copy(kind, p, 0, f).start()
                        relay_copy(kind, p, 1, f).start()
            if c == 1:
                take_mass(p, 1)
            wide(2 * c + 4)
            if c == 1:
                mass_copy(p, 2).start()
            wait_passed(p, c)
            wide(2 * c + 5)

        @pl.when(t == 0)
        def _():
            pltpu.make_async_copy(ev, ev, io_sem.at[2]).wait()
            for i in range(2):
                for half in range(2):
                    at = res.at[i, pl.ds(2 * half, 2)]
                    pltpu.make_async_copy(at, at, res_sem.at[i, half]).wait()

        take_mass(p, 2)

        def take(h, f):
            wait_relays(p, h, f)
            block_copy(S_D, p, h, f).start()

        def right(h, i, f):
            return g[p, h, DG + i, pl.ds(pl.multiple_of(f * KU, KU), KU)]

        def next_rows(h, c):
            at = pl.ds(c * KU, KU)
            line = (factor / nodes) * mass[p, 3, 0, :, h * 128:(h + 1) * 128]
            return factor * acc[h, at] + (1.0 - factor) * ev[h, at] + line

        def wait_all_sends():
            for h in range(2):
                wait_sends(p, h)
            at = mass.at[p, pl.ds(0, 3), 0]
            pltpu.make_async_remote_copy(src_ref=at, dst_ref=at, send_sem=msend.at[p], recv_sem=mrecv.at[p, 0],
                                         device_id=peer(SIB), device_id_type=MESH).wait_send()

        @pl.when(more)
        def _():
            for h in range(2):
                def narrow(*terms):
                    pieces = [right(h, i, f) for i, f in terms]
                    piece = jnp.concatenate(pieces, axis=0) if len(terms) > 1 else pieces[0]
                    for m in range(rows // MB):
                        mt = pl.ds(m * MB, MB)
                        left = [res[i, f, mt] for i, f in terms]
                        left = jnp.concatenate(left, axis=1) if len(terms) > 1 else left[0]
                        acc[h, mt] += jnp.dot(left, piece, preferred_element_type=jnp.float32)

                take(h, 0)
                narrow((0, 0))

                @pl.loop(1, 4)
                def _(f):
                    take(h, f)
                    block_copy(S_D, p, h, f - 1).wait_recv()
                    narrow((0, f), (1, f - 1))

                block_copy(S_D, p, h, 3).wait_recv()
                narrow((1, 3))

                part = jnp.zeros((8, 128), jnp.float32)
                for c in range(4):
                    at = pl.ds(c * KU, KU)
                    value = next_rows(h, c)
                    g[q, h, OWN, at] = value.astype(jnp.bfloat16)
                    part += fold(c, value)
                    acc[h, at] = jnp.zeros((KU, 128), jnp.float32)
                    if c in (1, 2):
                        send_own(q, h, c - 1)
                mass[q, 0, 0, :, h * 128:(h + 1) * 128] = jnp.sum(part, axis=0, keepdims=True)
            for h in range(2):
                send_own(q, h, 2, (S_OWN,))
            mass_copy(q, 0).start()
            wait_all_sends()
            for h in range(2):
                send_own(q, h, 3, (S_OWN,))

        @pl.when(jnp.logical_not(more))
        def _():
            def both(i, f, scale=None):
                piece = jnp.concatenate([right(h, i, f) for h in range(2)], axis=1)
                for m in range(rows // MB):
                    mt = pl.ds(m * MB, MB)
                    prod = jnp.dot(res[i, f, mt], piece, preferred_element_type=jnp.float32)
                    if scale is not None:
                        prod = scale * prod
                    acc[0, mt] += prod[:, :128]
                    acc[1, mt] += prod[:, 128:]

            def take_both(f):
                for h in range(2):
                    take(h, f)

            def wait_far(f):
                for h in range(2):
                    block_copy(S_D, p, h, f).wait_recv()

            @pl.loop(0, 3)
            def _(f):
                take_both(f)
                both(0, f)
                wait_far(f)
                both(1, f)

            for h in range(2):
                for c in range(4):
                    acc[h, pl.ds(c * KU, KU)] = next_rows(h, c)
            take_both(3)
            both(0, 3, factor)
            wait_far(3)
            both(1, 3, factor)
            wait_all_sends()

        return carry

    lax.fori_loop(0, num_sweeps, sweep, 0)


def finish(halves, out_hbm, sem):
    copies = [pltpu.make_async_copy(halves.at[h], out_hbm.at[:, pl.ds(h * 128, 128)], sem.at[h]) for h in range(2)]
    for copy in copies:
        copy.start()
    for copy in copies:
        copy.wait()


def solution(mesh):
    spec_rows = P(("batch", "row"), None)
    spec_vec = P(("batch", "row"))

    def local_sweeps(mat_rows, tele_rows, dang_rows, damping, start_rows):
        rows, nodes = mat_rows.shape
        seeds = start_rows.shape[1]
        num_sweeps = damping.shape[0]
        any_space = pl.BlockSpec(memory_space=pl.ANY)
        vmem = pl.BlockSpec(memory_space=pltpu.VMEM)
        sem = pltpu.SemaphoreType.DMA
        halves = pl.pallas_call(
            functools.partial(kernel, num_sweeps),
            out_shape=pltpu.VMEM((2, rows, 128), jnp.float32),
            in_specs=[any_space] * 5,
            out_specs=vmem,
            scratch_shapes=[
                pltpu.VMEM((2, 2, 8, rows, 128), jnp.bfloat16),
                pltpu.VMEM((RING, rows, 2 * KU), jnp.bfloat16),
                pltpu.VMEM((2, 4, rows, KU), jnp.bfloat16),
                pltpu.VMEM((2, rows, 128), jnp.float32),
                pltpu.VMEM((rows, 128), jnp.float32),
                pltpu.VMEM((rows // 128, 128), jnp.int32),
                pltpu.SMEM(damping.shape, jnp.float32),
                pltpu.VMEM((2, 4, 2, 1, 256), jnp.float32),
                sem((2, 2, 4)),
                sem((2, 4)),
                sem((2,)),
                sem((4,)),
                sem((2, 4)),
                sem((2, 2)),
                sem((2, 3)),
                sem((2,)),
                sem((RING,)),
                sem((2, 2)),
                sem((5,)),
            ],
            compiler_params=pltpu.CompilerParams(collective_id=0, has_side_effects=True, vmem_limit_bytes=KERNEL_VMEM),
            name="sweeps",
        )(mat_rows, tele_rows, dang_rows.reshape(rows // 128, 128), damping, start_rows)
        return pl.pallas_call(
            finish,
            out_shape=jax.ShapeDtypeStruct((rows, seeds), jnp.float32),
            in_specs=[vmem],
            out_specs=any_space,
            scratch_shapes=[sem((2,))],
            compiler_params=pltpu.CompilerParams(vmem_limit_bytes=8 << 20),
            name="finish",
        )(halves)

    return jax.shard_map(local_sweeps, mesh=mesh, in_specs=(spec_rows, spec_rows, spec_vec, P(None), spec_rows),
                         out_specs=spec_rows, check_vma=False)
```

```python
import functools

import jax
import jax.numpy as jnp
from jax import lax
from jax.experimental import pallas as pl
from jax.experimental.pallas import tpu as pltpu
from jax.sharding import PartitionSpec as P

MESH = pl.DeviceIdType.MESH
OWN, SIB, XN, XS, YN, YS, DG, DS = range(8)
X_OWN, Y_OWN, X_FWD, Y_FWD, S_OWN, S_X, S_Y, S_D = range(8)
RING = 6
UNITS = 12
KU = 512
FS = (384, 256, 256, 128)
FO = (0, 384, 640, 896)
MB = 512
NEAR = (SIB, XN, YN)
KERNEL_VMEM = 64487424


def flip(a, b):
    return a + b - 2 * a * b


def kernel(num_sweeps, a_hbm, e_hbm, d_hbm, damp_hbm, r_hbm, acc, g, ring, res, ev, dcol, dbuf, damp, mass,
           near_sem, relay_sem, sib_sem, pass_sem, far_sem, send, mrecv, msend, ring_sem, res_sem, io_sem):
    rows = acc.shape[1]
    nodes = a_hbm.shape[1]
    group = lax.axis_index("batch")
    me = lax.axis_index("row")
    core = lax.rem(me, 2)
    xpos = lax.rem(lax.div(me, 2), 2)
    ypos = lax.div(me, 4)

    def index_of(slot):
        sbit, xbit, ybit = slot & 1, (slot >> 1) & 1, (slot >> 2) & 1
        return (flip(ypos, ybit) * 2 + flip(xpos, xbit)) * 2 + flip(core, sbit)

    def peer(slot):
        return (group, index_of(slot))

    barrier = pltpu.get_barrier_semaphore()
    for slot in NEAR:
        pl.semaphore_signal(barrier, inc=1, device_id=peer(slot), device_id_type=MESH)

    def arrival(kind, p, h, c):
        if kind in (X_OWN, Y_OWN):
            return near_sem.at[p, h, c]
        if kind in (X_FWD, Y_FWD):
            return relay_sem.at[h, c]
        if kind == S_OWN:
            return sib_sem.at[c // 2]
        return far_sem.at[h, c] if kind == S_D else pass_sem.at[c]

    def remote(kind, p, h, c, src, dst):
        to = {X_OWN: XN, Y_OWN: YN, X_FWD: XN, Y_FWD: YN}.get(kind, SIB)
        return pltpu.make_async_remote_copy(src_ref=src, dst_ref=dst, send_sem=send.at[p, h],
                                            recv_sem=arrival(kind, p, h, c), device_id=peer(to), device_id_type=MESH)

    def far_rows(f):
        return pl.ds(2 * FO[f], 2 * FS[f])

    def block_copy(kind, p, h, c):
        src, dst = {X_OWN: (OWN, XN), Y_OWN: (OWN, YN), S_OWN: (OWN, SIB), S_X: (XN, XS), S_Y: (YN, YS),
                    S_D: (DG, DS)}[kind]
        at = far_rows(c) if kind == S_D else pl.ds(c * KU, KU)
        return remote(kind, p, h, c, g.at[p, h, src, at], g.at[p, h, dst, at])

    def relay_copy(kind, p, h, f):
        src, start, part = (YN, 0, 0) if kind == X_FWD else (XN, rows // 2, 1)
        return remote(kind, p, h, f, g.at[p, h, src, pl.ds(start + FO[f], FS[f])],
                      g.at[p, h, DG, pl.ds(2 * FO[f] + part * FS[f], FS[f])])

    def wait_near(p, h, c):
        at = g.at[p, h, pl.ds(0, 2), pl.ds(c * KU, KU)]
        remote(X_OWN, p, h, c, at, at).wait_recv()

    def wait_relays(p, h, f):
        at = g.at[p, h, DG, far_rows(f)]
        remote(X_FWD, p, h, f, at, at).wait_recv()

    def wait_sib(p, half):
        at = g.at[p, :, SIB, pl.ds(half * 2 * KU, 2 * KU)]
        remote(S_OWN, p, 0, 2 * half, at, at).wait_recv()

    def wait_passed(p, c):
        at = g.at[p, :, pl.ds(0, 2), pl.ds(c * KU, KU)]
        remote(S_X, p, 0, c, at, at).wait_recv()

    def wait_sends(p, h):
        at = g.at[p, h, pl.ds(0, 7)]
        remote(S_D, p, h, 0, at, at).wait_send()

    def parts_of(u):
        if u < 4:
            return [(u // 2, 2 * (u % 2)), (u // 2, 2 * (u % 2) + 1)]
        return [(slot, (u - 4) // 2) for slot in ((XN, YN) if u % 2 == 0 else (XS, YS))]

    def start_unit(u):
        parts = parts_of(u)
        if parts[0][0] == parts[1][0]:
            parts = [(parts[0][0], parts[0][1], 0, 2 * KU)]
        else:
            parts = [(slot, c, i * KU, KU) for i, (slot, c) in enumerate(parts)]
        for slot, c, to, size in parts:
            col = pl.multiple_of(index_of(slot) * rows + c * KU, KU)
            pltpu.make_async_copy(a_hbm.at[:, pl.ds(col, size)], ring.at[u % RING, :, pl.ds(to, size)],
                                  ring_sem.at[u % RING]).start()

    def wait_unit(u):
        at = ring.at[u % RING]
        pltpu.make_async_copy(at, at, ring_sem.at[u % RING]).wait()

    def res_copy(i, f, part):
        col = pl.multiple_of(index_of(DG + i) * rows + FO[f] + part * (rows // 2), 128)
        return pltpu.make_async_copy(a_hbm.at[:, pl.ds(col, FS[f])],
                                     res.at[i, :, pl.ds(2 * FO[f] + part * FS[f], FS[f])], res_sem.at[i])

    def half_copy(src, dst, h, sem):
        return pltpu.make_async_copy(src.at[:, pl.ds(h * 128, 128)], dst.at[h], sem)

    for h in range(2):
        half_copy(r_hbm, acc, h, io_sem.at[h]).start()
    d_copy = pltpu.make_async_copy(d_hbm, dbuf, io_sem.at[3])
    d_copy.start()
    damp_copy = pltpu.make_async_copy(damp_hbm, damp, io_sem.at[4])
    damp_copy.start()
    pl.semaphore_wait(barrier, 3)

    def send_own(p, h, c, kinds=(X_OWN, Y_OWN, S_OWN)):
        for kind in kinds:
            block_copy(kind, p, h, c).start()

    def mass_copy(p, i):
        return pltpu.make_async_remote_copy(src_ref=mass.at[p, i, 0], dst_ref=mass.at[p, i, 1],
                                            send_sem=msend.at[p], recv_sem=mrecv.at[p, i],
                                            device_id=peer(NEAR[i]), device_id_type=MESH)

    def take_mass(p, i):
        mass_copy(p, i).wait_recv()
        mass[p, i + 1, 0] = mass[p, i, 0] + mass[p, i, 1]

    def fold(c, value):
        weighed = value * dcol[pl.ds(c * KU, KU), :]
        return jnp.sum(weighed.reshape(KU // 8, 8, 128), axis=0)

    for h in range(2):
        half_copy(r_hbm, acc, h, io_sem.at[h]).wait()
        for c in range(4):
            at = pl.ds(c * KU, KU)
            g[0, h, OWN, at] = acc[h, at].astype(jnp.bfloat16)
            if h == 0 and c in (1, 2):
                send_own(0, 0, c - 1)
    for h, c in ((1, 0), (1, 1)):
        send_own(0, h, c)
    for h, c in ((0, 2), (1, 2), (0, 3), (1, 3)):
        send_own(0, h, c, (S_OWN,))

    for u in range(RING):
        start_unit(u)
    for h in range(2):
        half_copy(e_hbm, ev, h, io_sem.at[2]).start()
    for i in range(2):
        for f in range(4):
            for part in range(2):
                res_copy(i, f, part).start()
    d_copy.wait()
    for c in range(rows // 128):
        line = jnp.broadcast_to(dbuf[pl.ds(c, 1), :].astype(jnp.float32), (128, 128))
        dcol[pl.ds(c * 128, 128), :] = line.T
    for h in range(2):
        part = jnp.zeros((8, 128), jnp.float32)
        for c in range(4):
            part += fold(c, acc[h, pl.ds(c * KU, KU)])
        mass[0, 0, 0, :, h * 128:(h + 1) * 128] = jnp.sum(part, axis=0, keepdims=True)
        acc[h] = jnp.zeros_like(acc[h])
    mass_copy(0, 0).start()
    damp_copy.wait()

    def sweep(t, carry):
        p = lax.rem(t, 2)
        q = 1 - p
        more = t < num_sweeps - 1
        factor = damp[t]

        def wide(u):
            wait_unit(u)
            piece = jnp.concatenate(
                [jnp.concatenate([g[p, h, slot, pl.ds(c * KU, KU)] for h in range(2)], axis=1) for slot, c in parts_of(u)],
                axis=0)
            for m in range(rows // MB):
                mt = pl.ds(m * MB, MB)
                prod = jnp.dot(ring[u % RING, mt], piece, preferred_element_type=jnp.float32)
                acc[0, mt] += prod[:, :128]
                acc[1, mt] += prod[:, 128:]
            if u + RING < UNITS:
                start_unit(u + RING)
            else:
                @pl.when(more)
                def _():
                    start_unit(u + RING - UNITS)

        wide(0)
        take_mass(p, 0)
        for h in range(2):
            send_own(p, h, 2, (Y_OWN,))
        mass_copy(p, 1).start()
        for h, c, kind in ((0, 2, X_OWN), (1, 2, X_OWN), (0, 3, X_OWN), (0, 3, Y_OWN), (1, 3, X_OWN), (1, 3, Y_OWN)):
            send_own(p, h, c, (kind,))
        wide(1)
        for u in (2, 3):
            wait_sib(p, u - 2)
            wide(u)
        for c in range(4):
            for h in range(2):
                wait_near(p, h, c)
                block_copy(S_X, p, h, c).start()
                block_copy(S_Y, p, h, c).start()
                kind = X_FWD if c < 2 else Y_FWD
                here = (1, 2, 3) if c % 2 else (0,)

                @pl.when(more)
                def _():
                    for f in here if h == 0 else range(4 * (c % 2)):
                        relay_copy(kind, p, h, f).start()

                @pl.when(jnp.logical_not(more))
                def _():
                    for f in here if h == 1 else ():
                        relay_copy(kind, p, 0, f).start()
                        relay_copy(kind, p, 1, f).start()
            if c == 1:
                take_mass(p, 1)
            wide(2 * c + 4)
            if c == 1:
                mass_copy(p, 2).start()
            wait_passed(p, c)
            wide(2 * c + 5)

        @pl.when(t == 0)
        def _():
            pltpu.make_async_copy(ev, ev, io_sem.at[2]).wait()
            for i in range(2):
                pltpu.make_async_copy(res.at[i], res.at[i], res_sem.at[i]).wait()

        take_mass(p, 2)

        def take(h, f):
            wait_relays(p, h, f)
            block_copy(S_D, p, h, f).start()

        def right(h, i, f):
            return g[p, h, DG + i, far_rows(f)]

        def next_rows(h, c):
            at = pl.ds(c * KU, KU)
            line = (factor / nodes) * mass[p, 3, 0, :, h * 128:(h + 1) * 128]
            return factor * acc[h, at] + (1.0 - factor) * ev[h, at] + line

        def wait_all_sends():
            for h in range(2):
                wait_sends(p, h)
            at = mass.at[p, pl.ds(0, 3), 0]
            pltpu.make_async_remote_copy(src_ref=at, dst_ref=at, send_sem=msend.at[p], recv_sem=mrecv.at[p, 0],
                                         device_id=peer(SIB), device_id_type=MESH).wait_send()

        @pl.when(more)
        def _():
            for h in range(2):
                def narrow(*terms):
                    pieces = [right(h, i, f) for i, f in terms]
                    piece = jnp.concatenate(pieces, axis=0) if len(terms) > 1 else pieces[0]
                    for m in range(rows // MB):
                        mt = pl.ds(m * MB, MB)
                        left = [res[i, mt, far_rows(f)] for i, f in terms]
                        left = jnp.concatenate(left, axis=1) if len(terms) > 1 else left[0]
                        acc[h, mt] += jnp.dot(left, piece, preferred_element_type=jnp.float32)

                take(h, 0)
                narrow((0, 0))

                for f in range(1, 4):
                    take(h, f)
                    block_copy(S_D, p, h, f - 1).wait_recv()
                    narrow((0, f), (1, f - 1))

                block_copy(S_D, p, h, 3).wait_recv()
                narrow((1, 3))

                part = jnp.zeros((8, 128), jnp.float32)
                for c in range(4):
                    at = pl.ds(c * KU, KU)
                    value = next_rows(h, c)
                    g[q, h, OWN, at] = value.astype(jnp.bfloat16)
                    part += fold(c, value)
                    acc[h, at] = jnp.zeros((KU, 128), jnp.float32)
                    if c in (1, 2):
                        send_own(q, h, c - 1)
                mass[q, 0, 0, :, h * 128:(h + 1) * 128] = jnp.sum(part, axis=0, keepdims=True)
            for h in range(2):
                send_own(q, h, 2, (S_OWN,))
            mass_copy(q, 0).start()
            wait_all_sends()
            for h in range(2):
                send_own(q, h, 3, (S_OWN,))

        @pl.when(jnp.logical_not(more))
        def _():
            def both(i, f, scale=None):
                piece = jnp.concatenate([right(h, i, f) for h in range(2)], axis=1)
                for m in range(rows // MB):
                    mt = pl.ds(m * MB, MB)
                    prod = jnp.dot(res[i, mt, far_rows(f)], piece, preferred_element_type=jnp.float32)
                    if scale is not None:
                        prod = scale * prod
                    acc[0, mt] += prod[:, :128]
                    acc[1, mt] += prod[:, 128:]

            def take_both(f):
                for h in range(2):
                    take(h, f)

            def wait_far(f):
                for h in range(2):
                    block_copy(S_D, p, h, f).wait_recv()

            for f in range(3):
                take_both(f)
                both(0, f)
                wait_far(f)
                both(1, f)

            for h in range(2):
                for c in range(4):
                    acc[h, pl.ds(c * KU, KU)] = next_rows(h, c)
            take_both(3)
            both(0, 3, factor)
            wait_far(3)
            both(1, 3, factor)
            wait_all_sends()

        return carry

    lax.fori_loop(0, num_sweeps, sweep, 0)


def finish(halves, out_hbm, sem):
    copies = [pltpu.make_async_copy(halves.at[h], out_hbm.at[:, pl.ds(h * 128, 128)], sem.at[h]) for h in range(2)]
    for copy in copies:
        copy.start()
    for copy in copies:
        copy.wait()


def solution(mesh):
    spec_rows = P(("batch", "row"), None)
    spec_vec = P(("batch", "row"))

    def local_sweeps(mat_rows, tele_rows, dang_rows, damping, start_rows):
        rows, nodes = mat_rows.shape
        seeds = start_rows.shape[1]
        num_sweeps = damping.shape[0]
        any_space = pl.BlockSpec(memory_space=pl.ANY)
        vmem = pl.BlockSpec(memory_space=pltpu.VMEM)
        sem = pltpu.SemaphoreType.DMA
        halves = pl.pallas_call(
            functools.partial(kernel, num_sweeps),
            out_shape=pltpu.VMEM((2, rows, 128), jnp.float32),
            in_specs=[any_space] * 5,
            out_specs=vmem,
            scratch_shapes=[
                pltpu.VMEM((2, 2, 8, rows, 128), jnp.bfloat16),
                pltpu.VMEM((RING, rows, 2 * KU), jnp.bfloat16),
                pltpu.VMEM((2, rows, rows), jnp.bfloat16),
                pltpu.VMEM((2, rows, 128), jnp.float32),
                pltpu.VMEM((rows, 128), jnp.float32),
                pltpu.VMEM((rows // 128, 128), jnp.int32),
                pltpu.SMEM(damping.shape, jnp.float32),
                pltpu.VMEM((2, 4, 2, 1, 256), jnp.float32),
                sem((2, 2, 4)),
                sem((2, 4)),
                sem((2,)),
                sem((4,)),
                sem((2, 4)),
                sem((2, 2)),
                sem((2, 3)),
                sem((2,)),
                sem((RING,)),
                sem((2,)),
                sem((5,)),
            ],
            compiler_params=pltpu.CompilerParams(collective_id=0, has_side_effects=True, vmem_limit_bytes=KERNEL_VMEM),
            name="sweeps",
        )(mat_rows, tele_rows, dang_rows.reshape(rows // 128, 128), damping, start_rows)
        return pl.pallas_call(
            finish,
            out_shape=jax.ShapeDtypeStruct((rows, seeds), jnp.float32),
            in_specs=[vmem],
            out_specs=any_space,
            scratch_shapes=[sem((2,))],
            compiler_params=pltpu.CompilerParams(vmem_limit_bytes=8 << 20),
            name="finish",
        )(halves)

    return jax.shard_map(local_sweeps, mesh=mesh, in_specs=(spec_rows, spec_rows, spec_vec, P(None), spec_rows),
                         out_specs=spec_rows, check_vma=False)
```
